32 devices in a mesh: groups: 2 (over y), row: 4 (over z), col: 4 (over x, core).
Axes of the slice: x: 2, y: 2, z: 4, core: 2. Of those that a mesh axis runs over, the one named last changes fastest.
Arguments:
- factors: float32 [8, 1280, 5120], P('groups', 'row', 'col'), parts along dimension 0, may hold values from -1.5 to 1.5, as said below
- right_side: float32 [8, 1280, 96], P(('groups', 'col'), 'row'), parts along dimension 0, may hold values from -6 to 6
Outputs:
- forward: float32 [8, 1280, 96], P(('groups', 'col'), 'row'), parts along dimension 0
- solution: float32 [8, 1280, 96], P(('groups', 'col'), 'row'), parts along dimension 0
The draws below stay inside these ranges and needn't reach their ends.
There are 2 independent parts, one for each index of `groups`. The reference program is written for one: setup_inputs(seed, part) draws one part's arguments, and reference() takes and returns one part's arrays. A program takes and returns all parts, laid end to end along the dimension named above; each array names one. Nothing has to cross between parts.
Inputs may be any that keep to these rules, and one draw needn't show every extreme that they name: `factors`: off the diagonal tiles, the entries are those of L below and of U above. Diagonal tile k holds, strictly below its diagonal, the strictly lower part of the inverse of L's unit lower triangular diagonal tile, and on and above its diagonal the inverse of U's upper triangular diagonal tile.
All inputs are finite; a program needn't handle non-finite values.
Results may differ from the reference program's by a relative error of at most 0.00014.
Values sent between devices are 32-bit elements; how exact they have to be, the bound alone decides.
A program may use at most 128 MiB of HBM per device.

```python
import math
import jax
import jax.numpy as jnp
from jax import lax

TS = 1280
R = 96
TILES = 4


def draw_factors(key, part):
    first, second = jax.random.split(jax.random.fold_in(key, 11))
    shape = (TILES, TS, TILES * TS)
    base = jnp.clip(jax.random.normal(first, shape, jnp.float32), -4.0, 4.0)
    pivots = jax.random.uniform(second, shape, jnp.float32, 0.5, 1.5)
    tile_ids = jnp.arange(TILES)[:, None, None]
    inner = jnp.arange(TS)[None, :, None]
    columns = jnp.arange(TILES * TS)[None, None, :]
    same = columns // TS == tile_ids
    local = columns % TS
    scaled = jnp.where(same, base * (0.5 / math.sqrt(TS)), base * (1.0 / math.sqrt(TILES * TS)))
    return jnp.where(same & (local == inner), pivots, scaled)


def level_of(rng, dims, cuts, low, top_value):
    loudness, own = 1.0, jax.random.fold_in(rng, 6)
    for dim, parts in cuts:
        steps = jnp.exp(jax.random.uniform(jax.random.fold_in(own, dim), (parts,), jnp.float32, low / len(cuts), top_value / len(cuts)))
        loudness = loudness * jnp.repeat(steps, dims[dim] // parts).reshape([-1 if axis == dim else 1 for axis in range(len(dims))])
    return loudness


def gaussian(rng, shape, spread, reach, pieces=(), kind=jnp.bfloat16):
    result = jax.random.normal(rng, shape, jnp.float32) * spread
    if len(pieces) > 0:
        result = level_of(rng, shape, pieces, -0.22, 0.18) * result
    return jnp.clip(result, min=-reach, max=reach).astype(kind)


def setup_inputs(seed: int = 0, part: int = 0) -> dict:
    splits = jax.random.split(jax.random.key(seed), 3)
    part_keys = jax.random.split(jax.random.fold_in(splits[2], part), 3)
    return {
        "factors": draw_factors(jax.random.fold_in(jax.random.fold_in(splits[2], part), 71), part),
        "right_side": gaussian(part_keys[1], (TILES, TS, R), 1.0, 6.0, ((0, 4), (1, 4)), jnp.float32),
    }


def reference(factors, right_side):
    row_ids = jnp.arange(TS)[:, None]
    col_ids = jnp.arange(TS)[None, :]
    forward = []
    for current in range(TILES):
        vector = right_side[current]
        if current > 0:
            earlier = jnp.concatenate(forward, 0)
            vector = vector - jnp.dot(factors[current, :, :current * TS], earlier, preferred_element_type=jnp.float32, precision=lax.Precision.HIGHEST)
        diagonal = factors[current, :, current * TS:(current + 1) * TS]
        lower = jnp.where(col_ids < row_ids, diagonal, 0.0) + (col_ids == row_ids).astype(diagonal.dtype)
        forward.append(jnp.dot(lower, vector, preferred_element_type=jnp.float32, precision=lax.Precision.HIGHEST))
    solution = [None] * TILES
    for current in range(TILES - 1, -1, -1):
        vector = forward[current]
        if current < TILES - 1:
            later = jnp.concatenate(solution[current + 1:], 0)
            vector = vector - jnp.dot(factors[current, :, (current + 1) * TS:], later, preferred_element_type=jnp.float32, precision=lax.Precision.HIGHEST)
        diagonal = factors[current, :, current * TS:(current + 1) * TS]
        upper = jnp.where(col_ids >= row_ids, diagonal, 0.0)
        solution[current] = jnp.dot(upper, vector, preferred_element_type=jnp.float32, precision=lax.Precision.HIGHEST)
    return jnp.stack(forward), jnp.stack(solution)
```

```python
import functools

import jax
import jax.numpy as jnp
from jax import lax
from jax.experimental import pallas as pl
from jax.experimental.pallas import tpu as pltpu
from jax.sharding import PartitionSpec as P

MESH = pl.DeviceIdType.MESH
CHUNKS = 3


def kernel(
    n_row, n_col, chunks,
    ahi_hbm, alo_hbm, rs_ref,
    fwd_ref, sol_ref,
    ahi, alo, v_buf, f_buf, w_buf, s_buf, t_buf, tb_buf, rin, rout, rbin, rbout,
    a_sem, v_send, v_recv, f_send, f_recv, w_send, w_recv, s_send, s_recv,
    r_send, r_recv, rb_send, rb_recv, b0_send,
):
    r = lax.axis_index("row")
    c = lax.axis_index("col")
    last = n_col - 1

    def load(i, k):
        return (
            pltpu.make_async_copy(ahi_hbm.at[k], ahi.at[k], a_sem.at[0, k]),
            pltpu.make_async_copy(alo_hbm.at[k], alo.at[k], a_sem.at[1, k]),
        )

    def start_load(i, _):
        k = lax.rem(c + i, n_col + 1)
        for copy in load(i, k):
            copy.start()
        return 0

    lax.fori_loop(0, n_col + 1, start_load, 0)

    def wait_load(k):
        for copy in load(0, k):
            copy.wait()

    barrier = pltpu.get_barrier_semaphore()

    def greet(i, _):
        rr, cc = i // n_col, i % n_col

        @pl.when(i != r * n_col + c)
        def _():
            pl.semaphore_signal(barrier, inc=1, device_id={"row": rr, "col": cc}, device_id_type=MESH)

        return 0

    lax.fori_loop(0, n_row * n_col, greet, 0)
    pl.semaphore_wait(barrier, n_row * n_col - 1)

    def remote(src, dst, send, recv, row, col):
        return pltpu.make_async_remote_copy(
            src_ref=src, dst_ref=dst, send_sem=send, recv_sem=recv,
            device_id={"row": row, "col": col}, device_id_type=MESH,
        )

    def around(d):
        half = (d + 1) // 2
        odd = d % 2
        return lax.rem(r + odd * half - (1 - odd) * half + n_row, n_row)

    def each_chunk(body):
        def step(q, _):
            body(q)
            return 0

        lax.fori_loop(0, chunks, step, 0)

    def each_row(body, first=0):
        def step(d, _):
            body(around(d))
            return 0

        lax.fori_loop(first, n_row, step, 0, unroll=n_row <= 4)

    def part(x, k, s):
        hi = x.astype(jnp.bfloat16)
        lo = (x - hi.astype(jnp.float32)).astype(jnp.bfloat16)
        both = jnp.concatenate([hi, lo], axis=0)
        dims = (((1,), (1,)), ((), ()))
        m = x.shape[0]
        one = lax.dot_general(both, ahi[k, s], dims, preferred_element_type=jnp.float32)
        two = lax.dot_general(hi, alo[k, s], dims, preferred_element_type=jnp.float32)
        return one[:m] + one[m:] + two

    def combine(buf, k, q, wait):
        def step(d, acc):
            s = around(d)
            if wait is not None:
                wait(q, s)
            return acc + part(buf[q, s], k, s)

        zero = jnp.zeros(buf.shape[2:], jnp.float32)
        return lax.fori_loop(0, n_row, step, zero, unroll=n_row <= 4)

    def arrival(buf, recv):
        def wait(q, s):
            remote(buf.at[q, s], buf.at[q, s], recv.at[q, s], recv.at[q, s], r, c).wait_recv()

        return wait

    def arrival_but_own(buf, recv):
        inner = arrival(buf, recv)

        def wait(q, s):
            @pl.when(s != r)
            def _():
                inner(q, s)

        return wait

    def to_row(src, buf, send, recv, q, row):
        return remote(src, buf.at[q, r], send.at[q, row], recv.at[q, r], row, c)

    @pl.when(c == 0)
    def _():
        def one(q):
            v_buf[q, r] = rs_ref[q]
            each_row(lambda row: to_row(rs_ref.at[q], v_buf, v_send, v_recv, q, row).start(), 1)

        each_chunk(one)

    def first_run(q):
        return remote(rs_ref.at[q], rin.at[c, q], r_send.at[c, q], r_recv.at[c, q], r, 0)

    @pl.when(c > 0)
    def _():
        each_chunk(lambda q: first_run(q).start())

    wait_load(c)

    def back_run(q):
        return remote(f_buf.at[q, r], rbin.at[c, q], b0_send.at[q], rb_recv.at[c, q], r, last)

    def solve_forward(wait):
        def one(q):
            acc = combine(v_buf, c, q, wait)
            f_buf[q, r] = acc
            each_row(lambda row: to_row(f_buf.at[q, r], f_buf, f_send, f_recv, q, row).start(), 1)

            @pl.when(c < last)
            def _():
                back_run(q).start()

            fwd_ref[q] = acc

        each_chunk(one)

    @pl.when(c == 0)
    def _():
        solve_forward(arrival_but_own(v_buf, v_recv))

    @pl.when(c > 0)
    def _():
        solve_forward(arrival(v_buf, v_recv))

    def wait_run(run, recv, k, q):
        remote(run.at[k, q], run.at[k, q], recv.at[k, q], recv.at[k, q], r, c).wait_recv()

    def sweep(buf, recv, first, count, step, run_in, run_recv, run_out, run_send, stage, out, send, out_recv):
        nxt = c + step
        wait = arrival_but_own(buf, recv)
        wait_load(first)

        def one(q):
            acc = combine(buf, first, q, wait)
            wait_run(run_in, run_recv, first, q)
            stage[q] = run_in[first, q] - acc
            each_row(
                lambda row: remote(stage.at[q], out.at[q, r], send.at[q, row], out_recv.at[q, r], row, nxt).start()
            )

        each_chunk(one)

        def other(i, _):
            k = first + step * i
            wait_load(k)

            def inner(q):
                acc = combine(buf, k, q, None)
                wait_run(run_in, run_recv, k, q)
                run_out[k, q] = run_in[k, q] - acc
                remote(run_out.at[k, q], run_in.at[k, q], run_send.at[k, q], run_recv.at[k, q], r, nxt).start()

            each_chunk(inner)
            return 0

        lax.fori_loop(1, count, other, 0)

    @pl.when(c < last)
    def _():
        sweep(f_buf, f_recv, c + 1, last - c, 1, rin, r_recv, rout, r_send, t_buf, v_buf, w_send, v_recv)

    wait_load(n_col)

    def solve_backward(buf, wait):
        def one(q):
            acc = combine(buf, n_col, q, wait)
            s_buf[q, r] = acc

            @pl.when(c > 0)
            def _():
                each_row(lambda row: to_row(s_buf.at[q, r], s_buf, s_send, s_recv, q, row).start(), 1)

            sol_ref[q] = acc

        each_chunk(one)

    @pl.when(c == last)
    def _():
        solve_backward(f_buf, arrival_but_own(f_buf, f_recv))

    @pl.when(c < last)
    def _():
        solve_backward(w_buf, arrival(w_buf, w_recv))

    @pl.when(c > 0)
    def _():
        sweep(s_buf, s_recv, c - 1, c, -1, rbin, rb_recv, rbout, rb_send, tb_buf, w_buf, v_send, w_recv)

    def sent(src, send):
        remote(src, src, send, send, r, c).wait_send()

    def finish(q):
        @pl.when(c == 0)
        def _():
            each_row(lambda row: sent(rs_ref.at[q], v_send.at[q, row]), 1)

        @pl.when(c > 0)
        def _():
            sent(rs_ref.at[q], r_send.at[c, q])
            each_row(lambda row: sent(tb_buf.at[q], v_send.at[q, row]))
            each_row(lambda row: sent(s_buf.at[q, r], s_send.at[q, row]), 1)

        each_row(lambda row: sent(f_buf.at[q, r], f_send.at[q, row]), 1)

        @pl.when(c < last)
        def _():
            sent(f_buf.at[q, r], b0_send.at[q])
            each_row(lambda row: sent(t_buf.at[q], w_send.at[q, row]))

        def run(k, _):
            @pl.when(k > c + 1)
            def _():
                sent(rout.at[k, q], r_send.at[k, q])

            @pl.when(k < c - 1)
            def _():
                sent(rbout.at[k, q], rb_send.at[k, q])

            return 0

        lax.fori_loop(0, n_col, run, 0)

    each_chunk(finish)


def local(n_row, n_col, factors, right_side):
    tiles, rows, size = factors.shape
    width = right_side.shape[2]
    chunks = CHUNKS
    portion = width // chunks
    padded = -(-rows // 128) * 128
    column = lax.axis_index("col")
    row_index = lax.axis_index("row")

    tile_ids = jnp.arange(tiles)[:, None, None]
    global_rows = row_index * rows + jnp.arange(rows)[None, :, None]
    global_cols = jnp.arange(size)[None, None, :]
    lower = jnp.where(global_cols < global_rows, factors, 0.0) + (global_cols == global_rows).astype(jnp.float32)
    packed = jnp.where(tile_ids == column, lower, factors)
    diagonal = lax.dynamic_index_in_dim(factors, column, 0, keepdims=True)
    upper = jnp.where(global_cols >= global_rows, diagonal, 0.0)

    def arranged(a):
        a = a.reshape(a.shape[0], rows, n_row, rows).transpose(0, 2, 1, 3)
        return jnp.pad(a, ((0, 0), (0, 0), (0, padded - rows), (0, padded - rows)))

    whole = jnp.concatenate([arranged(packed), arranged(upper)], axis=0)
    high = lax.reduce_precision(whole, 8, 7)
    ahi = high.astype(jnp.bfloat16)
    alo = (whole - high).astype(jnp.bfloat16)

    rs = jnp.pad(right_side[0].T, ((0, 0), (0, padded - rows))).reshape(chunks, portion, padded)

    vmem = pl.BlockSpec(memory_space=pltpu.VMEM)
    anywhere = pl.BlockSpec(memory_space=pl.ANY)
    gathered = pltpu.VMEM((chunks, n_row, portion, padded), jnp.float32)
    staged = pltpu.VMEM((chunks, portion, padded), jnp.float32)
    runs = pltpu.VMEM((tiles, chunks, portion, padded), jnp.float32)
    weights = pltpu.VMEM((tiles + 1, n_row, padded, padded), jnp.bfloat16)
    dma = pltpu.SemaphoreType.DMA
    shape = jax.ShapeDtypeStruct((chunks, portion, padded), jnp.float32)
    fwd, sol = pl.pallas_call(
        functools.partial(kernel, n_row, n_col, chunks),
        out_shape=(shape, shape),
        in_specs=[anywhere, anywhere, vmem],
        out_specs=(vmem, vmem),
        scratch_shapes=[
            weights, weights, gathered, gathered, gathered, gathered, staged, staged, runs, runs, runs, runs,
            dma((2, tiles + 1)),
            *([dma((chunks, n_row))] * 8),
            *([dma((tiles, chunks))] * 4),
            dma((chunks,)),
        ],
        compiler_params=pltpu.CompilerParams(collective_id=0, has_side_effects=True, vmem_limit_bytes=60 << 20),
    )(ahi, alo, rs)

    def back(y):
        return y.reshape(width, padded)[:, :rows].T[None]

    return back(fwd), back(sol)


def solution(mesh):
    return jax.shard_map(
        functools.partial(local, mesh.shape["row"], mesh.shape["col"]),
        mesh=mesh,
        in_specs=(P("groups", "row", "col"), P(("groups", "col"), "row", None)),
        out_specs=(P(("groups", "col"), "row", None), P(("groups", "col"), "row", None)),
        check_vma=False,
    )
```

```python
import functools

import jax
import jax.numpy as jnp
from jax import lax
from jax.experimental import pallas as pl
from jax.experimental.pallas import tpu as pltpu
from jax.sharding import PartitionSpec as P

MESH = pl.DeviceIdType.MESH
CHUNKS = 3


def kernel(
    n_row, n_col, chunks, rows, size, width, window, depth,
    factors_hbm, rs_ref,
    fwd_ref, sol_ref,
    raw, ahi, alo, rs_pad, out_pad, rs_buf, v_buf, f_buf, w_buf, s_buf, t_buf, tb_buf, rin, rout, rbin, rbout,
    a_sem, v_send, v_recv, f_send, f_recv, w_send, w_recv, s_send, s_recv,
    r_send, r_recv, rb_send, rb_recv, b0_send,
):
    r = lax.axis_index("row")
    c = lax.axis_index("col")
    last = n_col - 1
    start = r * rows
    shift = pl.multiple_of(start % 128, 8)

    def load(k):
        dst = raw.at[k, pl.ds(shift, rows), pl.ds(0, size)]
        return pltpu.make_async_copy(factors_hbm.at[k], dst, a_sem.at[k])

    def start_load(i, _):
        load(lax.rem(c + i, n_col)).start()
        return 0

    lax.fori_loop(0, n_col, start_load, 0)

    barrier = pltpu.get_barrier_semaphore()

    def greet(i, _):
        rr, cc = i // n_col, i % n_col

        @pl.when(i != r * n_col + c)
        def _():
            pl.semaphore_signal(barrier, inc=1, device_id={"row": rr, "col": cc}, device_id_type=MESH)

        return 0

    lax.fori_loop(0, n_row * n_col, greet, 0)
    pl.semaphore_wait(barrier, n_row * n_col - 1)

    def remote(src, dst, send, recv, row, col):
        return pltpu.make_async_remote_copy(
            src_ref=src, dst_ref=dst, send_sem=send, recv_sem=recv,
            device_id={"row": row, "col": col}, device_id_type=MESH,
        )

    def around(d):
        half = (d + 1) // 2
        odd = d % 2
        return lax.rem(r + odd * half - (1 - odd) * half + n_row, n_row)

    def each_chunk(body):
        def step(q, _):
            body(q)
            return 0

        lax.fori_loop(0, chunks, step, 0)

    def each_row(body, first=0):
        def step(d, _):
            body(around(d))
            return 0

        lax.fori_loop(first, n_row, step, 0, unroll=n_row <= 4)

    def part(x, k, s):
        columns = pl.ds(pl.multiple_of((s * rows) // 128 * 128, 128), window)
        hi = x.astype(jnp.bfloat16)
        lo = (x - hi.astype(jnp.float32)).astype(jnp.bfloat16)
        both = jnp.concatenate([hi, lo], axis=0)
        dims = (((1,), (1,)), ((), ()))
        m = x.shape[0]
        one = lax.dot_general(both, ahi[k, :, columns], dims, preferred_element_type=jnp.float32)
        two = lax.dot_general(hi, alo[k, :, columns], dims, preferred_element_type=jnp.float32)
        return one[:m] + one[m:] + two

    def combine(buf, k, q, wait):
        def step(d, acc):
            s = around(d)
            if wait is not None:
                wait(q, s)
            return acc + part(buf[q, s], k, s)

        zero = jnp.zeros(buf.shape[2:], jnp.float32)
        return lax.fori_loop(0, n_row, step, zero, unroll=n_row <= 4)

    def arrival(buf, recv):
        def wait(q, s):
            remote(buf.at[q, s], buf.at[q, s], recv.at[q, s], recv.at[q, s], r, c).wait_recv()

        return wait

    def arrival_but_own(buf, recv):
        inner = arrival(buf, recv)

        def wait(q, s):
            @pl.when(s != r)
            def _():
                inner(q, s)

        return wait

    def to_row(src, buf, send, recv, q, row):
        return remote(src, buf.at[q, r], send.at[q, row], recv.at[q, r], row, c)

    portion = width // chunks
    rs_pad[...] = jnp.zeros(rs_pad.shape, jnp.float32)
    rs_pad[pl.ds(shift, rows), :width] = rs_ref[0]
    turned = rs_pad[...].T
    for q in range(chunks):
        rs_buf[q] = turned[q * portion : (q + 1) * portion]

    def deliver(buf, out_ref):
        whole = jnp.concatenate([buf[q, r] for q in range(chunks)], axis=0)
        spare = out_pad.shape[1] - width
        if spare:
            whole = jnp.concatenate([whole, jnp.zeros((spare, window), jnp.float32)], axis=0)
        out_pad[...] = whole.T
        out_ref[0] = out_pad[pl.ds(shift, rows), :width]

    @pl.when(c == 0)
    def _():
        def one(q):
            v_buf[q, r] = rs_buf[q]
            each_row(lambda row: to_row(rs_buf.at[q], v_buf, v_send, v_recv, q, row).start(), 1)

        each_chunk(one)

    def first_run(q):
        return remote(rs_buf.at[q], rin.at[c, q], r_send.at[c, q], r_recv.at[c, q], r, 0)

    @pl.when(c > 0)
    def _():
        each_chunk(lambda q: first_run(q).start())

    block = 16

    def split(src, dst, kind):
        def step(i, _):
            base = pl.multiple_of(i * block, block)
            line = lax.broadcasted_iota(jnp.int32, (block, depth), 0) + (base - shift)
            place = lax.broadcasted_iota(jnp.int32, (block, depth), 1)
            value = raw[src, pl.ds(base, block), :]
            keep = (line >= 0) & (line < rows) & (place < size)
            if kind == 1:
                value = jnp.where(place == line + start, 1.0, value)
                keep = keep & (place <= line + start)
            if kind == 2:
                keep = keep & (place >= line + start)
            value = jnp.where(keep, value, 0.0)
            hi = value.astype(jnp.bfloat16)
            ahi[dst, pl.ds(base, block), :] = hi
            alo[dst, pl.ds(base, block), :] = (value - hi.astype(jnp.float32)).astype(jnp.bfloat16)
            return 0

        lax.fori_loop(0, window // block, step, 0)

    def split_others():
        def step(i, _):
            k = lax.rem(c + i, n_col)
            load(k).wait()
            split(k, k, 0)
            return 0

        lax.fori_loop(1, n_col, step, 0)
        split(c, n_col, 2)

    load(c).wait()
    split(c, c, 1)

    @pl.when(c > 0)
    def _():
        split_others()

    def back_run(q):
        return remote(f_buf.at[q, r], rbin.at[c, q], b0_send.at[q], rb_recv.at[c, q], r, last)

    def solve_forward(wait):
        def one(q):
            acc = combine(v_buf, c, q, wait)
            f_buf[q, r] = acc
            each_row(lambda row: to_row(f_buf.at[q, r], f_buf, f_send, f_recv, q, row).start(), 1)

            @pl.when(c < last)
            def _():
                back_run(q).start()

        each_chunk(one)

    @pl.when(c == 0)
    def _():
        solve_forward(arrival_but_own(v_buf, v_recv))

    @pl.when(c > 0)
    def _():
        solve_forward(arrival(v_buf, v_recv))

    deliver(f_buf, fwd_ref)

    @pl.when(c == 0)
    def _():
        split_others()

    def wait_run(run, recv, k, q):
        remote(run.at[k, q], run.at[k, q], recv.at[k, q], recv.at[k, q], r, c).wait_recv()

    def sweep(buf, recv, first, count, step, run_in, run_recv, run_out, run_send, stage, out, send, out_recv):
        nxt = c + step
        wait = arrival_but_own(buf, recv)

        def one(q):
            acc = combine(buf, first, q, wait)
            wait_run(run_in, run_recv, first, q)
            stage[q] = run_in[first, q] - acc
            each_row(
                lambda row: remote(stage.at[q], out.at[q, r], send.at[q, row], out_recv.at[q, r], row, nxt).start()
            )

        each_chunk(one)

        def other(i, _):
            k = first + step * i

            def inner(q):
                acc = combine(buf, k, q, None)
                wait_run(run_in, run_recv, k, q)
                run_out[k, q] = run_in[k, q] - acc
                remote(run_out.at[k, q], run_in.at[k, q], run_send.at[k, q], run_recv.at[k, q], r, nxt).start()

            each_chunk(inner)
            return 0

        lax.fori_loop(1, count, other, 0)

    @pl.when(c < last)
    def _():
        sweep(f_buf, f_recv, c + 1, last - c, 1, rin, r_recv, rout, r_send, t_buf, v_buf, w_send, v_recv)


    def solve_backward(buf, wait):
        def one(q):
            acc = combine(buf, n_col, q, wait)
            s_buf[q, r] = acc

            @pl.when(c > 0)
            def _():
                each_row(lambda row: to_row(s_buf.at[q, r], s_buf, s_send, s_recv, q, row).start(), 1)


        each_chunk(one)

    @pl.when(c == last)
    def _():
        solve_backward(f_buf, arrival_but_own(f_buf, f_recv))

    @pl.when(c < last)
    def _():
        solve_backward(w_buf, arrival(w_buf, w_recv))

    @pl.when(c > 0)
    def _():
        sweep(s_buf, s_recv, c - 1, c, -1, rbin, rb_recv, rbout, rb_send, tb_buf, w_buf, v_send, w_recv)

    deliver(s_buf, sol_ref)

    def sent(src, send):
        remote(src, src, send, send, r, c).wait_send()

    def finish(q):
        @pl.when(c == 0)
        def _():
            each_row(lambda row: sent(rs_buf.at[q], v_send.at[q, row]), 1)

        @pl.when(c > 0)
        def _():
            sent(rs_buf.at[q], r_send.at[c, q])
            each_row(lambda row: sent(tb_buf.at[q], v_send.at[q, row]))
            each_row(lambda row: sent(s_buf.at[q, r], s_send.at[q, row]), 1)

        each_row(lambda row: sent(f_buf.at[q, r], f_send.at[q, row]), 1)

        @pl.when(c < last)
        def _():
            sent(f_buf.at[q, r], b0_send.at[q])
            each_row(lambda row: sent(t_buf.at[q], w_send.at[q, row]))

        def run(k, _):
            @pl.when(k > c + 1)
            def _():
                sent(rout.at[k, q], r_send.at[k, q])

            @pl.when(k < c - 1)
            def _():
                sent(rbout.at[k, q], rb_send.at[k, q])

            return 0

        lax.fori_loop(0, n_col, run, 0)

    each_chunk(finish)


def local(n_row, n_col, factors, right_side):
    tiles, rows, size = factors.shape
    width = right_side.shape[2]
    chunks = CHUNKS
    portion = width // chunks
    starts = [i * rows for i in range(n_row)]
    window = max(-(-(i % 128 + rows) // 128) * 128 for i in starts)
    depth = max(max(i // 128 * 128 + window for i in starts), size)
    lanes = -(-width // 128) * 128

    vmem = pl.BlockSpec(memory_space=pltpu.VMEM)
    anywhere = pl.BlockSpec(memory_space=pl.ANY)
    gathered = pltpu.VMEM((chunks, n_row, portion, window), jnp.float32)
    staged = pltpu.VMEM((chunks, portion, window), jnp.float32)
    runs = pltpu.VMEM((tiles, chunks, portion, window), jnp.float32)
    weights = pltpu.VMEM((tiles + 1, window, depth), jnp.bfloat16)
    turning = pltpu.VMEM((window, lanes), jnp.float32)
    dma = pltpu.SemaphoreType.DMA
    shape = jax.ShapeDtypeStruct(right_side.shape, jnp.float32)
    return pl.pallas_call(
        functools.partial(kernel, n_row, n_col, chunks, rows, size, width, window, depth),
        out_shape=(shape, shape),
        in_specs=[anywhere, vmem],
        out_specs=(vmem, vmem),
        scratch_shapes=[
            pltpu.VMEM((tiles, window, depth), jnp.float32), weights, weights, turning, turning, staged,
            gathered, gathered, gathered, gathered, staged, staged, runs, runs, runs, runs,
            dma((tiles,)),
            *([dma((chunks, n_row))] * 8),
            *([dma((tiles, chunks))] * 4),
            dma((chunks,)),
        ],
        compiler_params=pltpu.CompilerParams(collective_id=0, has_side_effects=True, vmem_limit_bytes=60 << 20),
    )(factors, right_side)


def solution(mesh):
    return jax.shard_map(
        functools.partial(local, mesh.shape["row"], mesh.shape["col"]),
        mesh=mesh,
        in_specs=(P("groups", "row", "col"), P(("groups", "col"), "row", None)),
        out_specs=(P(("groups", "col"), "row", None), P(("groups", "col"), "row", None)),
        check_vma=False,
    )
```

```python
import functools

import jax
import jax.numpy as jnp
from jax import lax
from jax.experimental import pallas as pl
from jax.experimental.pallas import tpu as pltpu
from jax.sharding import PartitionSpec as P

MESH = pl.DeviceIdType.MESH
CHUNKS = 4


def kernel(
    n_row, n_col, chunks, rows, size, width, window, depth,
    factors_hbm, rs_ref,
    fwd_ref, sol_ref,
    raw, ahi, alo, rs_pad, out_pad, rs_buf, v_buf, f_buf, w_buf, s_buf, t_buf, tb_buf, rin, rout, rbin, rbout,
    a_sem, v_send, v_recv, f_send, f_recv, w_send, w_recv, s_send, s_recv,
    r_send, r_recv, rb_send, rb_recv, b0_send,
):
    r = lax.axis_index("row")
    c = lax.axis_index("col")
    last = n_col - 1
    start = r * rows
    shift = pl.multiple_of(start % 128, 8)

    def load(k):
        dst = raw.at[k, pl.ds(shift, rows), pl.ds(0, size)]
        return pltpu.make_async_copy(factors_hbm.at[k], dst, a_sem.at[k])

    def start_load(i, _):
        load(lax.rem(c + i, n_col)).start()
        return 0

    lax.fori_loop(0, n_col, start_load, 0)

    barrier = pltpu.get_barrier_semaphore()

    def greet(i, _):
        rr, cc = i // n_col, i % n_col

        @pl.when(i != r * n_col + c)
        def _():
            pl.semaphore_signal(barrier, inc=1, device_id={"row": rr, "col": cc}, device_id_type=MESH)

        return 0

    lax.fori_loop(0, n_row * n_col, greet, 0)
    pl.semaphore_wait(barrier, n_row * n_col - 1)

    def remote(src, dst, send, recv, row, col):
        return pltpu.make_async_remote_copy(
            src_ref=src, dst_ref=dst, send_sem=send, recv_sem=recv,
            device_id={"row": row, "col": col}, device_id_type=MESH,
        )

    def around(d):
        half = (d + 1) // 2
        odd = d % 2
        return lax.rem(r + odd * half - (1 - odd) * half + n_row, n_row)

    def each_chunk(body):
        def step(q, _):
            body(q)
            return 0

        lax.fori_loop(0, chunks, step, 0)

    def each_row(body, first=0):
        def step(d, _):
            body(around(d))
            return 0

        lax.fori_loop(first, n_row, step, 0, unroll=n_row <= 4)

    def part(x, k, s):
        columns = pl.ds(pl.multiple_of((s * rows) // 128 * 128, 128), window)
        hi = x.astype(jnp.bfloat16)
        lo = (x - hi.astype(jnp.float32)).astype(jnp.bfloat16)
        both = jnp.concatenate([hi, lo], axis=0)
        dims = (((1,), (1,)), ((), ()))
        m = x.shape[0]
        one = lax.dot_general(both, ahi[k, :, columns], dims, preferred_element_type=jnp.float32)
        two = lax.dot_general(hi, alo[k, :, columns], dims, preferred_element_type=jnp.float32)
        return one[:m] + one[m:] + two

    def combine(buf, k, q, wait):
        def step(d, acc):
            s = around(d)
            if wait is not None:
                wait(q, s)
            return acc + part(buf[q, s], k, s)

        zero = jnp.zeros(buf.shape[2:], jnp.float32)
        return lax.fori_loop(0, n_row, step, zero, unroll=n_row <= 4)

    def arrival(buf, recv):
        def wait(q, s):
            remote(buf.at[q, s], buf.at[q, s], recv.at[q, s], recv.at[q, s], r, c).wait_recv()

        return wait

    def arrival_but_own(buf, recv):
        inner = arrival(buf, recv)

        def wait(q, s):
            @pl.when(s != r)
            def _():
                inner(q, s)

        return wait

    def to_row(src, buf, send, recv, q, row):
        return remote(src, buf.at[q, r], send.at[q, row], recv.at[q, r], row, c)

    portion = width // chunks
    rs_pad[...] = jnp.zeros(rs_pad.shape, jnp.float32)
    rs_pad[pl.ds(shift, rows), :width] = rs_ref[0]
    turned = rs_pad[...].T
    for q in range(chunks):
        rs_buf[q] = turned[q * portion : (q + 1) * portion]

    def deliver(buf, out_ref):
        whole = jnp.concatenate([buf[q, r] for q in range(chunks)], axis=0)
        spare = out_pad.shape[1] - width
        if spare:
            whole = jnp.concatenate([whole, jnp.zeros((spare, window), jnp.float32)], axis=0)
        out_pad[...] = whole.T
        out_ref[0] = out_pad[pl.ds(shift, rows), :width]

    @pl.when(c == 0)
    def _():
        def one(q):
            v_buf[q, r] = rs_buf[q]
            each_row(lambda row: to_row(rs_buf.at[q], v_buf, v_send, v_recv, q, row).start(), 1)

        each_chunk(one)

    def first_run(q):
        return remote(rs_buf.at[q], rin.at[c, q], r_send.at[c, q], r_recv.at[c, q], r, 0)

    @pl.when(c > 0)
    def _():
        each_chunk(lambda q: first_run(q).start())

    block = 16

    def split(src, dst, kind):
        def step(i, _):
            base = pl.multiple_of(i * block, block)
            line = lax.broadcasted_iota(jnp.int32, (block, depth), 0) + (base - shift)
            place = lax.broadcasted_iota(jnp.int32, (block, depth), 1)
            value = raw[src, pl.ds(base, block), :]
            keep = (line >= 0) & (line < rows) & (place < size)
            if kind == 1:
                value = jnp.where(place == line + start, 1.0, value)
                keep = keep & (place <= line + start)
            if kind == 2:
                keep = keep & (place >= line + start)
            value = jnp.where(keep, value, 0.0)
            hi = value.astype(jnp.bfloat16)
            ahi[dst, pl.ds(base, block), :] = hi
            alo[dst, pl.ds(base, block), :] = (value - hi.astype(jnp.float32)).astype(jnp.bfloat16)
            return 0

        lax.fori_loop(0, window // block, step, 0)

    def split_others():
        def step(i, _):
            k = lax.rem(c + i, n_col)
            load(k).wait()
            split(k, k, 0)
            return 0

        lax.fori_loop(1, n_col, step, 0)
        split(c, n_col, 2)

    load(c).wait()
    split(c, c, 1)

    @pl.when(c > 0)
    def _():
        split_others()

    def back_run(q):
        return remote(f_buf.at[q, r], rbin.at[c, q], b0_send.at[q], rb_recv.at[c, q], r, last)

    def solve_forward(wait):
        def one(q):
            acc = combine(v_buf, c, q, wait)
            f_buf[q, r] = acc
            each_row(lambda row: to_row(f_buf.at[q, r], f_buf, f_send, f_recv, q, row).start(), 1)

            @pl.when(c < last)
            def _():
                back_run(q).start()

        each_chunk(one)

    @pl.when(c == 0)
    def _():
        solve_forward(arrival_but_own(v_buf, v_recv))

    @pl.when(c > 0)
    def _():
        solve_forward(arrival(v_buf, v_recv))

    deliver(f_buf, fwd_ref)

    @pl.when(c == 0)
    def _():
        split_others()

    def wait_run(run, recv, k, q):
        remote(run.at[k, q], run.at[k, q], recv.at[k, q], recv.at[k, q], r, c).wait_recv()

    def sweep(buf, recv, first, count, step, run_in, run_recv, run_out, run_send, stage, out, send, out_recv):
        nxt = c + step
        wait = arrival_but_own(buf, recv)

        def one(q):
            acc = combine(buf, first, q, wait)
            wait_run(run_in, run_recv, first, q)
            stage[q] = run_in[first, q] - acc
            each_row(
                lambda row: remote(stage.at[q], out.at[q, r], send.at[q, row], out_recv.at[q, r], row, nxt).start()
            )

        each_chunk(one)

        def other(i, _):
            k = first + step * i

            def inner(q):
                acc = combine(buf, k, q, None)
                wait_run(run_in, run_recv, k, q)
                run_out[k, q] = run_in[k, q] - acc
                remote(run_out.at[k, q], run_in.at[k, q], run_send.at[k, q], run_recv.at[k, q], r, nxt).start()

            each_chunk(inner)
            return 0

        lax.fori_loop(1, count, other, 0)

    @pl.when(c < last)
    def _():
        sweep(f_buf, f_recv, c + 1, last - c, 1, rin, r_recv, rout, r_send, t_buf, v_buf, w_send, v_recv)


    def solve_backward(buf, wait):
        def one(q):
            acc = combine(buf, n_col, q, wait)
            s_buf[q, r] = acc

            @pl.when(c > 0)
            def _():
                each_row(lambda row: to_row(s_buf.at[q, r], s_buf, s_send, s_recv, q, row).start(), 1)


        each_chunk(one)

    @pl.when(c == last)
    def _():
        solve_backward(f_buf, arrival_but_own(f_buf, f_recv))

    @pl.when(c < last)
    def _():
        solve_backward(w_buf, arrival(w_buf, w_recv))

    @pl.when(c > 0)
    def _():
        sweep(s_buf, s_recv, c - 1, c, -1, rbin, rb_recv, rbout, rb_send, tb_buf, w_buf, v_send, w_recv)

    deliver(s_buf, sol_ref)

    def sent(src, send):
        remote(src, src, send, send, r, c).wait_send()

    def finish(q):
        @pl.when(c == 0)
        def _():
            each_row(lambda row: sent(rs_buf.at[q], v_send.at[q, row]), 1)

        @pl.when(c > 0)
        def _():
            sent(rs_buf.at[q], r_send.at[c, q])
            each_row(lambda row: sent(tb_buf.at[q], v_send.at[q, row]))
            each_row(lambda row: sent(s_buf.at[q, r], s_send.at[q, row]), 1)

        each_row(lambda row: sent(f_buf.at[q, r], f_send.at[q, row]), 1)

        @pl.when(c < last)
        def _():
            sent(f_buf.at[q, r], b0_send.at[q])
            each_row(lambda row: sent(t_buf.at[q], w_send.at[q, row]))

        def run(k, _):
            @pl.when(k > c + 1)
            def _():
                sent(rout.at[k, q], r_send.at[k, q])

            @pl.when(k < c - 1)
            def _():
                sent(rbout.at[k, q], rb_send.at[k, q])

            return 0

        lax.fori_loop(0, n_col, run, 0)

    each_chunk(finish)


def local(n_row, n_col, factors, right_side):
    tiles, rows, size = factors.shape
    width = right_side.shape[2]
    chunks = CHUNKS
    portion = width // chunks
    starts = [i * rows for i in range(n_row)]
    window = max(-(-(i % 128 + rows) // 128) * 128 for i in starts)
    depth = max(max(i // 128 * 128 + window for i in starts), size)
    lanes = -(-width // 128) * 128

    vmem = pl.BlockSpec(memory_space=pltpu.VMEM)
    anywhere = pl.BlockSpec(memory_space=pl.ANY)
    gathered = pltpu.VMEM((chunks, n_row, portion, window), jnp.float32)
    staged = pltpu.VMEM((chunks, portion, window), jnp.float32)
    runs = pltpu.VMEM((tiles, chunks, portion, window), jnp.float32)
    weights = pltpu.VMEM((tiles + 1, window, depth), jnp.bfloat16)
    turning = pltpu.VMEM((window, lanes), jnp.float32)
    dma = pltpu.SemaphoreType.DMA
    shape = jax.ShapeDtypeStruct(right_side.shape, jnp.float32)
    return pl.pallas_call(
        functools.partial(kernel, n_row, n_col, chunks, rows, size, width, window, depth),
        out_shape=(shape, shape),
        in_specs=[anywhere, vmem],
        out_specs=(vmem, vmem),
        scratch_shapes=[
            pltpu.VMEM((tiles, window, depth), jnp.float32), weights, weights, turning, turning, staged,
            gathered, gathered, gathered, gathered, staged, staged, runs, runs, runs, runs,
            dma((tiles,)),
            *([dma((chunks, n_row))] * 8),
            *([dma((tiles, chunks))] * 4),
            dma((chunks,)),
        ],
        compiler_params=pltpu.CompilerParams(collective_id=0, has_side_effects=True, vmem_limit_bytes=60 << 20),
    )(factors, right_side)


def solution(mesh):
    return jax.shard_map(
        functools.partial(local, mesh.shape["row"], mesh.shape["col"]),
        mesh=mesh,
        in_specs=(P("groups", "row", "col"), P(("groups", "col"), "row", None)),
        out_specs=(P(("groups", "col"), "row", None), P(("groups", "col"), "row", None)),
        check_vma=False,
    )
```
